256 devices in a mesh: slab: 16 (over y_hi, z), sub: 16 (over x, y_lo, core).
Axes of the slice: x: 4, y: 4 (y_hi: 2, y_lo: 2; y = y_hi * 2 + y_lo), z: 8, core: 2. Of those that a mesh axis runs over, the one named last changes fastest.
Arguments:
- features: bfloat16 [64, 256, 49, 128], P('slab', 'sub'), may hold values from -6 to 6
- source_cell: int32 [16, 16, 2, 128], P('slab', 'sub'), may hold values from 42 to 117, as said below
- target_cell: int32 [16, 16, 2, 128], P('slab', 'sub'), may hold values from 0 to 159, as said below
- rotation: bfloat16 [16, 16, 2, 128, 455], P('slab', 'sub'), may hold values from -4 to 4
- edge_count: int32 [16, 16], P('slab', 'sub'), may hold values from 64 to 256, as said below
- first_zero: bfloat16 [896, 896], replicated, may hold values from -0.1875 to 0.1875
- first_one: bfloat16 [2, 768, 768], replicated, may hold values from -0.15625 to 0.15625
- first_two: bfloat16 [2, 640, 640], replicated, may hold values from -0.15625 to 0.15625
- second_zero: bfloat16 [896, 896], replicated, may hold values from -0.1875 to 0.1875
- second_one: bfloat16 [2, 768, 768], replicated, may hold values from -0.15625 to 0.15625
- second_two: bfloat16 [2, 640, 640], replicated, may hold values from -0.15625 to 0.15625
Outputs:
- aggregated: bfloat16 [64, 256, 49, 128], P('slab', 'sub')
The draws below stay inside these ranges and needn't reach their ends.
Inputs may be any that keep to these rules, and one draw needn't show every extreme that they name: source_cell names an atom of the device's own 4 x 16 block, as a cell of its window numbered row by row. target_cell names an atom other than the source, at most 2 atom rows and 2 atom columns from it. Slots at positions edge_count and beyond are unused; in every draw some device holds 256 live slots.
All inputs are finite; a program needn't handle non-finite values.
Results may differ from the reference program's by a relative error of at most 0.0074.
Values may be sent and summed in bfloat16 or wider, within the bound.
A program may use at most 128 MiB of HBM per device.

```python
import math
import jax
import jax.numpy as jnp
from jax import lax

CHANNELS = 128
DEGREE = 6
ROWS = 4
COLS = 16
REACH = 2
TILE = 128
TILES = 2
COMPS = 49
WIGNER = 455
ATOM_ROWS = 64
ATOM_COLS = 256
N_SLAB = 16
N_SUB = 16


def edge_cells(key):
    grid_shape = (N_SLAB, N_SUB, TILES, TILE)
    key_list = jax.random.split(jax.random.fold_in(key, 71), 4)
    atom_row = jax.random.randint(key_list[0], grid_shape, 0, ROWS)
    atom_col = jax.random.randint(key_list[1], grid_shape, 0, COLS)
    step_row = jax.random.randint(key_list[2], grid_shape, -REACH, REACH + 1)
    step_col = jax.random.randint(key_list[3], grid_shape, -REACH, REACH)
    step_col = jnp.where((step_row == 0) & (step_col >= 0), step_col + 1, step_col)
    atom_row = atom_row.at[0, 0, 0, 0].set(0).at[0, 0, 0, 1].set(ROWS - 1)
    atom_col = atom_col.at[0, 0, 0, 0].set(0).at[0, 0, 0, 1].set(COLS - 1)
    step_row = step_row.at[0, 0, 0, 0].set(-REACH).at[0, 0, 0, 1].set(REACH)
    step_col = step_col.at[0, 0, 0, 0].set(-REACH).at[0, 0, 0, 1].set(REACH - 1)
    wide_cols = COLS + 2 * REACH
    source = (atom_row + REACH) * wide_cols + atom_col + REACH
    target = (atom_row + step_row + REACH) * wide_cols + atom_col + step_col + REACH
    return (source.astype(jnp.int32), target.astype(jnp.int32))


def draw_source_cell(key, part):
    return edge_cells(key)[0]


def draw_target_cell(key, part):
    return edge_cells(key)[1]


def draw_edge_count(key, part):
    key_list = jax.random.split(jax.random.fold_in(key, 5), 3)
    most_edges = TILES * TILE
    base = jax.random.randint(key_list[0], (N_SLAB, N_SUB), TILE // 2, most_edges // 2 + 1)
    crowded = jax.random.randint(key_list[1], (N_SLAB, N_SUB), 0, 3) == 0
    counts = jnp.where(crowded, base * 2, base).reshape(-1)
    fullest = jax.random.randint(key_list[2], (), 0, N_SLAB * N_SUB)
    counts = jnp.where(jnp.arange(N_SLAB * N_SUB) == fullest, most_edges, counts)
    return counts.reshape(N_SLAB, N_SUB).astype(jnp.int32)


def levels(key, dims, cuts, low, top_value):
    level = 1.0
    for axis_at, parts in cuts:
        heights = jax.random.uniform(jax.random.fold_in(jax.random.fold_in(key, 6), axis_at), (parts,), jnp.float32, low / len(cuts), top_value / len(cuts))
        level = level * jnp.repeat(jnp.exp(heights), dims[axis_at] // parts).reshape((-1,) + (1,) * (len(dims) - 1 - axis_at))
    return level


def gaussian(rng, dims, scale, most, cuts=(), kind=jnp.bfloat16):
    loudness = levels(rng, dims, cuts, -0.22, 0.18) if cuts else 1.0
    entries = jax.random.normal(rng, dims, jnp.float32) * scale * loudness
    return jnp.minimum(jnp.maximum(entries, -most), most).astype(kind)


def setup_inputs(seed: int = 0) -> dict:
    streams_of = jax.random.split(jax.random.key(seed), 12)
    return {
        "features": gaussian(streams_of[0], (ATOM_ROWS, ATOM_COLS, COMPS, CHANNELS), 1.0, 6.0, ((0, 16), (1, 16))),
        "source_cell": draw_source_cell(jax.random.fold_in(streams_of[11], 71), 0),
        "target_cell": draw_target_cell(jax.random.fold_in(streams_of[11], 71), 0),
        "rotation": gaussian(streams_of[3], (N_SLAB, N_SUB, TILES, TILE, WIGNER), 1.0, 4.0, ((0, 16), (1, 16))),
        "edge_count": draw_edge_count(jax.random.fold_in(streams_of[11], 71), 0),
        "first_zero": gaussian(streams_of[5], ((DEGREE + 1) * CHANNELS, (DEGREE + 1) * CHANNELS), ((DEGREE + 1) * CHANNELS) ** -0.5, 0.1875),
        "first_one": gaussian(streams_of[6], (2, DEGREE * CHANNELS, DEGREE * CHANNELS), (2 * DEGREE * CHANNELS) ** -0.5, 0.15625),
        "first_two": gaussian(streams_of[7], (2, (DEGREE - 1) * CHANNELS, (DEGREE - 1) * CHANNELS), (2 * (DEGREE - 1) * CHANNELS) ** -0.5, 0.15625),
        "second_zero": gaussian(streams_of[8], ((DEGREE + 1) * CHANNELS, (DEGREE + 1) * CHANNELS), ((DEGREE + 1) * CHANNELS) ** -0.5, 0.1875),
        "second_one": gaussian(streams_of[9], (2, DEGREE * CHANNELS, DEGREE * CHANNELS), (2 * DEGREE * CHANNELS) ** -0.5, 0.15625),
        "second_two": gaussian(streams_of[10], (2, (DEGREE - 1) * CHANNELS, (DEGREE - 1) * CHANNELS), (2 * (DEGREE - 1) * CHANNELS) ** -0.5, 0.15625),
    }


exact_mode = lax.Precision.HIGHEST

def block_of(frames, degree):
    offset = sum(((2 * lower_degree + 1) ** 2 for lower_degree in range(degree)))
    block_width = 2 * degree + 1
    return frames[:, offset:offset + block_width * block_width].reshape(frames.shape[0], block_width, block_width)

def turn_in(edge_input, frames):
    edge_rows = edge_input.shape[0]
    zero_rows, plus_one, minus_one, plus_two, minus_two = ([], [], [], [], [])
    for degree in range(DEGREE + 1):
        wigner_piece = block_of(frames, degree).astype(jnp.float32)
        inputs_piece = edge_input[:, degree * degree:(degree + 1) * (degree + 1), :].astype(jnp.float32)
        turned = jnp.einsum('eij,ejc->eic', wigner_piece, inputs_piece, precision=exact_mode) / math.sqrt(2 * degree + 1)
        zero_rows.append(turned[:, degree])
        if degree >= 1:
            plus_one.append(turned[:, degree + 1])
            minus_one.append(turned[:, degree - 1])
        if degree >= 2:
            plus_two.append(turned[:, degree + 2])
            minus_two.append(turned[:, degree - 2])
    order_zero = jnp.stack(zero_rows, 1).reshape(edge_rows, -1).astype(jnp.bfloat16)
    order_one = jnp.concatenate([jnp.stack(plus_one, 1), jnp.stack(minus_one, 1)], 0).reshape(2 * edge_rows, -1).astype(jnp.bfloat16)
    order_two = jnp.concatenate([jnp.stack(plus_two, 1), jnp.stack(minus_two, 1)], 0).reshape(2 * edge_rows, -1).astype(jnp.bfloat16)
    return (order_zero, order_one, order_two)

def convolve(order_zero, order_one, order_two, w_zero, w_one, w_two):
    edge_rows = order_zero.shape[0]
    results = [jnp.dot(order_zero, w_zero, preferred_element_type=jnp.float32)]
    for pair_in, w_pair in ((order_one, w_one), (order_two, w_two)):
        former = jnp.dot(pair_in, w_pair[0], preferred_element_type=jnp.float32)
        latter = jnp.dot(pair_in, w_pair[1], preferred_element_type=jnp.float32)
        results.append(former[:edge_rows] - latter[edge_rows:])
        results.append(former[edge_rows:] + latter[:edge_rows])
    return results

def activate(results, channels):
    edge_rows = results[0].shape[0]
    zero_part = results[0].reshape(edge_rows, -1, channels)
    scalar = zero_part[:, 0]
    gating = jax.nn.sigmoid(scalar)[:, None, :]
    zero_part = jnp.concatenate([jax.nn.silu(scalar)[:, None, :], zero_part[:, 1:] * gating], 1)
    shaped = [piece_out.reshape(edge_rows, -1, channels) * gating for piece_out in results[1:]]
    order_zero = zero_part.reshape(edge_rows, -1).astype(jnp.bfloat16)
    order_one = jnp.concatenate([shaped[0], shaped[1]], 0).reshape(2 * edge_rows, -1).astype(jnp.bfloat16)
    order_two = jnp.concatenate([shaped[2], shaped[3]], 0).reshape(2 * edge_rows, -1).astype(jnp.bfloat16)
    return (order_zero, order_one, order_two)

def turn_out(results, frames, channels):
    edge_rows = results[0].shape[0]
    zero_part, plus_one, minus_one, plus_two, minus_two = [piece_out.reshape(edge_rows, -1, channels) for piece_out in results]
    pieces = []
    for degree in range(DEGREE + 1):
        row_list = [zero_part[:, degree]]
        if degree >= 1:
            row_list = [minus_one[:, degree - 1]] + row_list + [plus_one[:, degree - 1]]
        if degree >= 2:
            row_list = [minus_two[:, degree - 2]] + row_list + [plus_two[:, degree - 2]]
        spread = len(row_list) // 2
        wigner_piece = block_of(frames, degree).astype(jnp.float32)[:, degree - spread:degree + spread + 1, :]
        column = jnp.stack(row_list, 1)
        pieces.append(jnp.einsum('eji,ejc->eic', wigner_piece, column, precision=exact_mode) / math.sqrt(2 * degree + 1))
    return jnp.concatenate(pieces, 1).astype(jnp.bfloat16)

def message(edge_input, frames, weights):
    channels = edge_input.shape[-1]
    order_zero, order_one, order_two = turn_in(edge_input, frames)
    results = convolve(order_zero, order_one, order_two, weights[0], weights[1], weights[2])
    order_zero, order_one, order_two = activate(results, channels)
    results = convolve(order_zero, order_one, order_two, weights[3], weights[4], weights[5])
    return turn_out(results, frames, channels)

def edge_inputs(window_cells, from_cell, to_cell):
    return (window_cells[from_cell].astype(jnp.float32) + window_cells[to_cell].astype(jnp.float32)).astype(jnp.bfloat16)

def deposit(messages, to_cell, is_live, cell_total):
    places = lax.broadcasted_iota(jnp.int32, (cell_total, to_cell.shape[0]), 0)
    one_hot = ((places == to_cell[None, :]) & is_live[None, :]).astype(jnp.bfloat16)
    return jnp.dot(one_hot, messages.reshape(messages.shape[0], -1), preferred_element_type=jnp.float32)

def reference(features, source_cell, target_cell, rotation, edge_count, first_zero, first_one, first_two, second_zero, second_one, second_two):
    weights = (first_zero, first_one, first_two, second_zero, second_one, second_two)
    components = features.shape[2]
    channels = features.shape[3]
    wide_rows = ROWS + 2 * REACH
    wide_cols = COLS + 2 * REACH
    cell_total = wide_rows * wide_cols
    padded = jnp.pad(features, ((REACH, REACH), (REACH, REACH), (0, 0), (0, 0)), mode='wrap')
    collected = jnp.zeros((ATOM_ROWS + 2 * REACH, ATOM_COLS + 2 * REACH, components * channels), jnp.float32)
    edge_lane = lax.iota(jnp.int32, TILE)
    zero_index = jnp.asarray(0, jnp.int32)

    def per_device(collected, device_index):
        device_index = jnp.asarray(device_index, jnp.int32)
        slab_index = device_index // N_SUB
        sub_index = device_index % N_SUB
        row_start = jnp.asarray(slab_index * ROWS, jnp.int32)
        col_start = jnp.asarray(sub_index * COLS, jnp.int32)
        window = lax.dynamic_slice(padded, (row_start, col_start, zero_index, zero_index), (wide_rows, wide_cols, components, channels))
        window_cells = window.reshape(cell_total, components, channels)
        sources = source_cell[slab_index, sub_index]
        targets = target_cell[slab_index, sub_index]
        frames_all = rotation[slab_index, sub_index]
        edge_total = edge_count[slab_index, sub_index].astype(jnp.int32)
        busy_tiles = (edge_total + TILE - 1) // TILE

        def one_tile(tile_index, window_sum):
            from_cell = sources[tile_index]
            to_cell = targets[tile_index]
            is_live = tile_index * TILE + edge_lane < edge_total
            messages = message(edge_inputs(window_cells, from_cell, to_cell), frames_all[tile_index], weights)
            return window_sum + deposit(messages, to_cell, is_live, cell_total)
        window_sum = lax.fori_loop(jnp.asarray(0, jnp.int32), busy_tiles, one_tile, jnp.zeros((cell_total, components * channels), jnp.float32))
        window_sum = window_sum.reshape(wide_rows, wide_cols, components * channels)
        corner = (row_start, col_start, zero_index)
        current = lax.dynamic_slice(collected, corner, window_sum.shape)
        return (lax.dynamic_update_slice(collected, current + window_sum, corner), None)
    collected, ignored = lax.scan(per_device, collected, jnp.arange(N_SLAB * N_SUB, dtype=jnp.int32))
    inner_sum = collected[:, REACH:REACH + ATOM_COLS]
    inner_sum = inner_sum.at[:, :REACH].add(collected[:, ATOM_COLS + REACH:])
    inner_sum = inner_sum.at[:, ATOM_COLS - REACH:].add(collected[:, :REACH])
    middle = inner_sum[REACH:REACH + ATOM_ROWS]
    middle = middle.at[:REACH].add(inner_sum[ATOM_ROWS + REACH:])
    middle = middle.at[ATOM_ROWS - REACH:].add(inner_sum[:REACH])
    return middle.reshape(ATOM_ROWS, ATOM_COLS, components, channels).astype(jnp.bfloat16)
```

```python
import math

import jax
import jax.numpy as jnp
import numpy as np
from jax import lax
from jax.experimental import pallas as pl
from jax.experimental.pallas import tpu as pltpu
from jax.sharding import PartitionSpec as P

DEGREE = 6
REACH = 2
COMPS = 49
WIGNER = 455
EDGES = 256
GROUP = 16
GROUPS = EDGES // GROUP
BF = jnp.bfloat16
F32 = jnp.float32


def spread_of(degree):
    return min(degree, 2)


def kept(degree):
    return 2 * spread_of(degree) + 1


FIRST_KEPT = [sum(kept(k) for k in range(d)) for d in range(DEGREE + 2)]
OFFSETS = [sum((2 * k + 1) ** 2 for k in range(d)) for d in range(DEGREE + 1)]


def entry_tables():
    inward = np.full((512,), -1, np.int32)
    outward = np.full((512,), -1, np.int32)
    row = 0
    for degree in range(DEGREE + 1):
        width = 2 * degree + 1
        spread = spread_of(degree)
        for slot, i in enumerate(range(degree - spread, degree + spread + 1)):
            for j in range(width):
                entry = OFFSETS[degree] + i * width + j
                inward[16 * row + j] = entry
                outward[8 * (degree * degree + j) + slot] = entry
            row += 1
    return np.concatenate([inward, outward])[None, :]


def transposed_dot(a, b):
    return lax.dot_general(a, b, (((0,), (0,)), ((), ())), preferred_element_type=F32)


def dot(a, b):
    return jnp.dot(a, b, preferred_element_type=F32)


def expand_rotations(table_ref, turn_ref, padded, grid_map, into, outof):
    wanted = table_ref[...]
    rows = lax.broadcasted_iota(jnp.int32, (WIGNER, 1024), 0)
    pick = jnp.where(rows == wanted, 1.0, 0.0).astype(BF)
    padded[...] = transposed_dot(turn_ref[...], pick).astype(BF)
    k = lax.broadcasted_iota(jnp.int32, (128, 2048), 0)
    col = lax.broadcasted_iota(jnp.int32, (128, 2048), 1)
    grid_map[...] = jnp.where(k == (col >> 4), 1.0, 0.0).astype(BF)
    edge = lax.broadcasted_iota(jnp.int32, (EDGES, 256), 0)
    lane = lax.broadcasted_iota(jnp.int32, (EDGES, 256), 1)
    own = (edge & 15) == (lane & 15)
    for degree in range(DEGREE + 1):
        lanes = 128 if degree <= 3 else 256
        for slot in range(kept(degree)):
            row = FIRST_KEPT[degree] + slot
            block = dot(
                padded[:, 128 * (row // 8) : 128 * (row // 8) + 128],
                grid_map[:, 256 * (row % 8) : 256 * (row % 8) + lanes],
            )
            into[degree][slot] = jnp.where(own[:, :lanes], block, 0.0).astype(BF)
    for pair in range((COMPS + 1) // 2):
        chunk, place = pair // 8, pair % 8
        block = dot(
            padded[:, 512 + 128 * chunk : 640 + 128 * chunk],
            grid_map[:, 256 * place : 256 * place + 256],
        )
        block = jnp.where(own, block, 0.0).astype(BF)
        outof[2 * pair] = block[:, :128]
        if 2 * pair + 1 < COMPS:
            outof[2 * pair + 1] = block[:, 128:]


def cell_numbers(shape):
    k = lax.broadcasted_iota(jnp.int32, shape, 0)
    own = ((k >> 4) + 2) * 20 + (k & 15) + 2
    r = (k - 64) >> 4
    slab = (jnp.where(r < 2, r, r + 4)) * 20 + (k & 15) + 2
    s = (k - 128) & 15
    side = (s >> 1) * 20 + (s & 1) + jnp.where(k >= 144, 18, 0)
    return jnp.where(k < 64, own, jnp.where(k < 128, slab, side))


def compute_kernel(
    own_ref,
    slab_ref,
    left_ref,
    right_ref,
    source_ref,
    target_ref,
    turn_ref,
    count_ref,
    table_ref,
    w0_hbm,
    w1_hbm,
    w2_hbm,
    w3_hbm,
    w4_hbm,
    w5_hbm,
    own_out,
    slab_out,
    left_out,
    right_out,
    w0,
    w1,
    w2,
    w3,
    w4,
    w5,
    padded,
    grid_map,
    i0,
    i1,
    i2,
    i3,
    i4,
    i5,
    i6,
    outof,
    gather_map,
    edges,
    zero_in,
    one_in,
    two_in,
    turned,
    sem,
):
    into = (i0, i1, i2, i3, i4, i5, i6)
    copies = [
        pltpu.make_async_copy(src, dst, sem.at[n])
        for n, (src, dst) in enumerate(
            ((w0_hbm, w0), (w1_hbm, w1), (w2_hbm, w2), (w3_hbm, w3), (w4_hbm, w4), (w5_hbm, w5))
        )
    ]
    for copy in copies:
        copy.start()
    expand_rotations(table_ref, turn_ref, padded, grid_map, into, outof)
    cells = cell_numbers((160, EDGES))
    to_target = jnp.where(cells == target_ref[...], 1.0, 0.0)
    both = to_target + jnp.where(cells == source_ref[...], 1.0, 0.0)
    gather_map[...] = both.T.astype(BF)

    def gather(step, carry):
        pieces = []
        for n in range(7):
            comp = step * 7 + n
            pieces.append(
                jnp.concatenate(
                    [
                        own_ref[:, comp].reshape(64, 128),
                        slab_ref[:, comp].reshape(64, 128),
                        left_ref[comp],
                        right_ref[comp],
                    ],
                    0,
                )
            )
        total = dot(gather_map[...], jnp.concatenate(pieces, 1)).astype(BF)
        for n in range(7):
            edges[step * 7 + n] = total[:, 128 * n : 128 * n + 128]
        return carry

    lax.fori_loop(0, 7, gather, 0)

    def turn_in(group, carry):
        at = pl.ds(pl.multiple_of(group * GROUP, GROUP), GROUP)
        low = pl.ds(pl.multiple_of(EDGES + group * GROUP, GROUP), GROUP)
        for degree in range(DEGREE + 1):
            width = 2 * degree + 1
            n = kept(degree)
            rows = edges[degree * degree : degree * degree + width, at, :]
            result = dot(
                into[degree][:, at, :].reshape(n * GROUP, -1)[:, : width * GROUP],
                rows.reshape(width * GROUP, 128),
            )
            result = result * (1.0 / math.sqrt(width))
            piece = [result[GROUP * k : GROUP * k + GROUP] for k in range(n)]
            mid = n // 2
            zero_in[at, 128 * degree : 128 * degree + 128] = piece[mid].astype(BF)
            if degree >= 1:
                c = 128 * (degree - 1)
                plus, minus = piece[mid + 1].astype(BF), piece[mid - 1]
                one_in[at, c : c + 128] = plus
                one_in[at, 768 + c : 896 + c] = (-minus).astype(BF)
                one_in[low, c : c + 128] = minus.astype(BF)
                one_in[low, 768 + c : 896 + c] = plus
            if degree >= 2:
                c = 128 * (degree - 2)
                plus, minus = piece[mid + 2].astype(BF), piece[mid - 2]
                two_in[at, c : c + 128] = plus
                two_in[at, 640 + c : 768 + c] = (-minus).astype(BF)
                two_in[low, c : c + 128] = minus.astype(BF)
                two_in[low, 640 + c : 768 + c] = plus
        return carry

    lax.fori_loop(0, GROUPS, turn_in, 0)
    for copy in copies[:3]:
        copy.wait()
    y0 = dot(zero_in[...], w0[...])
    scalar = y0[:, :128]
    gate = jax.nn.sigmoid(scalar)
    y1 = dot(one_in[...], w1[...])
    zero_in[:, :128] = (scalar * gate).astype(BF)
    for degree in range(1, DEGREE + 1):
        c = 128 * degree
        zero_in[:, c : c + 128] = (y0[:, c : c + 128] * gate).astype(BF)
    y2 = dot(two_in[...], w2[...])
    for y, ref, half in ((y1, one_in, 768), (y2, two_in, 640)):
        for c in range(0, half, 128):
            plus = y[:EDGES, c : c + 128] * gate
            minus = y[EDGES:, c : c + 128] * gate
            ref[:EDGES, c : c + 128] = plus.astype(BF)
            ref[:EDGES, half + c : half + c + 128] = (-minus).astype(BF)
            ref[EDGES:, c : c + 128] = minus.astype(BF)
            ref[EDGES:, half + c : half + c + 128] = plus.astype(BF)
    for copy in copies[3:]:
        copy.wait()
    u = dot(zero_in[...], w3[...])
    for degree in range(DEGREE + 1):
        scale = 1.0 / math.sqrt(2 * degree + 1)
        at = FIRST_KEPT[degree] + spread_of(degree)
        turned[at] = (u[:, 128 * degree : 128 * degree + 128] * scale).astype(BF)
    for m, ref, w in ((1, one_in, w4), (2, two_in, w5)):
        u = dot(ref[...], w[...])
        for degree in range(m, DEGREE + 1):
            scale = 1.0 / math.sqrt(2 * degree + 1)
            at = FIRST_KEPT[degree] + spread_of(degree)
            c = 128 * (degree - m)
            turned[at + m] = (u[:EDGES, c : c + 128] * scale).astype(BF)
            turned[at - m] = (u[EDGES:, c : c + 128] * scale).astype(BF)

    def turn_out(group, carry):
        at = pl.ds(pl.multiple_of(group * GROUP, GROUP), GROUP)
        for degree in range(DEGREE + 1):
            first, width, n = FIRST_KEPT[degree], 2 * degree + 1, kept(degree)
            result = dot(
                outof[degree * degree : degree * degree + width, at, :]
                .reshape(width * GROUP, 128)[:, : n * GROUP],
                turned[first : first + n, at, :].reshape(n * GROUP, 128),
            )
            edges[degree * degree : degree * degree + width, at, :] = result.astype(BF).reshape(
                width, GROUP, 128
            )
        return carry

    lax.fori_loop(0, GROUPS, turn_out, 0)
    lane = lax.broadcasted_iota(jnp.int32, (160, EDGES), 1)
    cells = cell_numbers((160, EDGES))
    scatter = jnp.where(
        (cells == target_ref[...]) & (lane < count_ref[0, 0]), 1.0, 0.0
    ).astype(BF)

    def deposit(step, carry):
        rows = jnp.concatenate([edges[step * 7 + n] for n in range(7)], 1)
        total = dot(scatter, rows)
        for n in range(7):
            comp = step * 7 + n
            part = total[:, 128 * n : 128 * n + 128]
            own_out[:, comp] = part[:64].reshape(4, 16, 128)
            slab_out[:, comp] = part[64:128].reshape(4, 16, 128)
            left_out[comp] = part[128:144].astype(BF)
            right_out[comp] = part[144:160].astype(BF)
        return carry

    lax.fori_loop(0, 7, deposit, 0)


def compute(own, slab, left, right, source, target, turn, count, table, weights):
    vmem = pl.BlockSpec(memory_space=pltpu.VMEM)
    smem = pl.BlockSpec(memory_space=pltpu.SMEM)
    anywhere = pl.BlockSpec(memory_space=pl.ANY)
    into = [
        pltpu.VMEM((kept(d), EDGES, 128 if d <= 3 else 256), BF) for d in range(DEGREE + 1)
    ]
    return pl.pallas_call(
        compute_kernel,
        out_shape=(
            jax.ShapeDtypeStruct((4, COMPS, 16, 128), F32),
            jax.ShapeDtypeStruct((4, COMPS, 16, 128), F32),
            jax.ShapeDtypeStruct((COMPS, 16, 128), BF),
            jax.ShapeDtypeStruct((COMPS, 16, 128), BF),
        ),
        in_specs=[vmem] * 7 + [smem, vmem] + [anywhere] * 6,
        out_specs=(vmem,) * 4,
        scratch_shapes=[pltpu.VMEM(w.shape, BF) for w in weights]
        + [pltpu.VMEM((EDGES, 1024), BF), pltpu.VMEM((128, 2048), BF)]
        + into
        + [
            pltpu.VMEM((COMPS, EDGES, 128), BF),
            pltpu.VMEM((EDGES, 160), BF),
            pltpu.VMEM((COMPS, EDGES, 128), BF),
            pltpu.VMEM((EDGES, 896), BF),
            pltpu.VMEM((2 * EDGES, 1536), BF),
            pltpu.VMEM((2 * EDGES, 1280), BF),
            pltpu.VMEM((FIRST_KEPT[-1], EDGES, 128), BF),
            pltpu.SemaphoreType.DMA((6,)),
        ],
        compiler_params=pltpu.CompilerParams(vmem_limit_bytes=60 * 1024 * 1024),
        cost_estimate=pl.CostEstimate(
            flops=12_000_000_000, bytes_accessed=20_000_000, transcendentals=40_000
        ),
        name="edge_messages",
    )(own, slab, left, right, source, target, turn, count, table, *weights)


def ring(axis, step):
    n = lax.axis_size(axis)
    return [(i, (i + step) % n) for i in range(n)]


def shift(x, axis, step):
    return lax.ppermute(x, axis, ring(axis, step))


def to_side(rows):
    return jnp.transpose(rows, (1, 0, 2, 3)).reshape(COMPS, 16, 128)


def from_side(side):
    return jnp.transpose(side.reshape(COMPS, 8, 2, 128), (1, 0, 2, 3))


def shards(features, source_cell, target_cell, rotation, edge_count, *weights):
    own = jnp.transpose(features, (0, 2, 1, 3))
    turn = jnp.transpose(rotation[0, 0], (2, 0, 1)).reshape(WIGNER, EDGES)
    weights = [w.reshape(-1, w.shape[-1]) for w in weights]
    low = shift(own[2:], "slab", 1)
    high = shift(own[:2], "slab", -1)
    tall = jnp.concatenate([low, own, high], 0)
    left = shift(to_side(tall[:, :, 14:]), "sub", 1)
    right = shift(to_side(tall[:, :, :2]), "sub", -1)
    slab = jnp.concatenate([low, high], 0)
    own_sum, slab_sum, left_sum, right_sum = compute(
        own,
        slab,
        left,
        right,
        source_cell.reshape(1, EDGES),
        target_cell.reshape(1, EDGES),
        turn,
        edge_count,
        jnp.asarray(entry_tables()),
        weights,
    )
    from_right = from_side(shift(left_sum, "sub", -1)).astype(F32)
    from_left = from_side(shift(right_sum, "sub", 1)).astype(F32)
    side = jnp.pad(from_right, ((0, 0), (0, 0), (14, 0), (0, 0))) + jnp.pad(
        from_left, ((0, 0), (0, 0), (0, 14), (0, 0))
    )
    slab_sum = (slab_sum + jnp.concatenate([side[:2], side[6:]], 0)).astype(BF)
    from_high = shift(slab_sum[:2], "slab", -1).astype(F32)
    from_low = shift(slab_sum[2:], "slab", 1).astype(F32)
    total = own_sum + side[2:6] + jnp.concatenate([from_low, from_high], 0)
    return jnp.transpose(total.astype(BF), (0, 2, 1, 3))


def solution(mesh):
    return jax.shard_map(
        shards,
        mesh=mesh,
        in_specs=(
            P("slab", "sub", None, None),
            P("slab", "sub", None, None),
            P("slab", "sub", None, None),
            P("slab", "sub", None, None, None),
            P("slab", "sub"),
            P(),
            P(),
            P(),
            P(),
            P(),
            P(),
        ),
        out_specs=P("slab", "sub", None, None),
        check_vma=False,
    )
```

```python
import math

import jax
import jax.numpy as jnp
import numpy as np
from jax import lax
from jax.experimental import pallas as pl
from jax.experimental.pallas import tpu as pltpu
from jax.sharding import PartitionSpec as P

DEGREE = 6
REACH = 2
COMPS = 49
WIGNER = 455
EDGES = 256
GROUP = 16
GROUPS = EDGES // GROUP
BF = jnp.bfloat16
F32 = jnp.float32


def spread_of(degree):
    return min(degree, 2)


def kept(degree):
    return 2 * spread_of(degree) + 1


FIRST_KEPT = [sum(kept(k) for k in range(d)) for d in range(DEGREE + 2)]
OFFSETS = [sum((2 * k + 1) ** 2 for k in range(d)) for d in range(DEGREE + 1)]


def entry_tables():
    inward = np.full((512,), -1, np.int32)
    outward = np.full((512,), -1, np.int32)
    row = 0
    for degree in range(DEGREE + 1):
        width = 2 * degree + 1
        spread = spread_of(degree)
        for slot, i in enumerate(range(degree - spread, degree + spread + 1)):
            for j in range(width):
                entry = OFFSETS[degree] + i * width + j
                inward[16 * row + j] = entry
                outward[8 * (degree * degree + j) + slot] = entry
            row += 1
    return np.concatenate([inward, outward])[None, :]


def transposed_dot(a, b):
    return lax.dot_general(a, b, (((0,), (0,)), ((), ())), preferred_element_type=F32)


def dot(a, b):
    return jnp.dot(a, b, preferred_element_type=F32)


def expand_rotations(table_ref, turn_ref, padded, grid_map, into, outof):
    wanted = table_ref[...]
    rows = lax.broadcasted_iota(jnp.int32, (WIGNER, 1024), 0)
    pick = jnp.where(rows == wanted, 1.0, 0.0).astype(BF)
    padded[...] = transposed_dot(turn_ref[...], pick).astype(BF)
    k = lax.broadcasted_iota(jnp.int32, (128, 2048), 0)
    col = lax.broadcasted_iota(jnp.int32, (128, 2048), 1)
    grid_map[...] = jnp.where(k == (col >> 4), 1.0, 0.0).astype(BF)
    edge = lax.broadcasted_iota(jnp.int32, (EDGES, 256), 0)
    lane = lax.broadcasted_iota(jnp.int32, (EDGES, 256), 1)
    own = (edge & 15) == (lane & 15)
    for degree in range(DEGREE + 1):
        lanes = 128 if degree <= 3 else 256
        for slot in range(kept(degree)):
            row = FIRST_KEPT[degree] + slot
            block = dot(
                padded[:, 128 * (row // 8) : 128 * (row // 8) + 128],
                grid_map[:, 256 * (row % 8) : 256 * (row % 8) + lanes],
            )
            into[degree][slot] = jnp.where(own[:, :lanes], block, 0.0).astype(BF)
    for pair in range((COMPS + 1) // 2):
        chunk, place = pair // 8, pair % 8
        block = dot(
            padded[:, 512 + 128 * chunk : 640 + 128 * chunk],
            grid_map[:, 256 * place : 256 * place + 256],
        )
        block = jnp.where(own, block, 0.0).astype(BF)
        outof[2 * pair] = block[:, :128]
        if 2 * pair + 1 < COMPS:
            outof[2 * pair + 1] = block[:, 128:]


def cell_numbers(shape, dim):
    k = lax.broadcasted_iota(jnp.int32, shape, dim)
    own = ((k >> 4) + 2) * 20 + (k & 15) + 2
    r = (k - 64) >> 4
    slab = (jnp.where(r < 2, r, r + 4)) * 20 + (k & 15) + 2
    s = (k - 128) & 15
    side = (s >> 1) * 20 + (s & 1) + jnp.where(k >= 144, 18, 0)
    return jnp.where(k < 64, own, jnp.where(k < 128, slab, side))


def rim_map(shape, cell_dim):
    cells = cell_numbers(shape, cell_dim)
    s = lax.broadcasted_iota(jnp.int32, shape, 1 - cell_dim)
    wanted = ((s & 15) >> 1) * 20 + (s & 1) + jnp.where(s < 16, 16, 2)
    return jnp.where(cells == wanted, 1.0, 0.0).astype(BF)


MESH = pl.DeviceIdType.MESH
IN_CHUNKS = ((6, 6), (0, 3), (5, 5), (4, 4))
OUT_CHUNKS = ((6, 6), (4, 5), (0, 3))
STEP = 4


def comps_of(chunk):
    return chunk[0] ** 2, (chunk[1] + 1) ** 2


def steps_of(chunk):
    lo, hi = comps_of(chunk)
    return [range(c, min(c + STEP, hi)) for c in range(lo, hi, STEP)]


def fused_kernel(
    own_hbm,
    source_ref,
    target_ref,
    turn_ref,
    count_ref,
    table_ref,
    w0_hbm,
    w1_hbm,
    w2_hbm,
    w3_hbm,
    w4_hbm,
    w5_hbm,
    out,
    own,
    slab,
    side,
    rim,
    w0,
    w1,
    w2,
    w3,
    w4,
    w5,
    padded,
    grid_map,
    i0,
    i1,
    i2,
    i3,
    i4,
    i5,
    i6,
    outof,
    gather_map,
    edges,
    zero_in,
    one_in,
    two_in,
    turned,
    summed,
    side_out,
    side_back,
    slab_out,
    slab_back,
    sem,
    in_sem,
    out_sem,
):
    into = (i0, i1, i2, i3, i4, i5, i6)
    load_own = pltpu.make_async_copy(own_hbm, own, sem.at[6])
    load_own.start()
    weights = [
        pltpu.make_async_copy(src, dst, sem.at[n])
        for n, (src, dst) in enumerate(
            ((w0_hbm, w0), (w1_hbm, w1), (w2_hbm, w2), (w3_hbm, w3), (w4_hbm, w4), (w5_hbm, w5))
        )
    ]
    a, b = lax.axis_index("slab"), lax.axis_index("sub")
    rows, cols = lax.axis_size("slab"), lax.axis_size("sub")
    up, down = (lax.rem(a + 1, rows), b), (lax.rem(a + rows - 1, rows), b)
    right, left = (a, lax.rem(b + 1, cols)), (a, lax.rem(b + cols - 1, cols))
    barrier = pltpu.get_barrier_semaphore()
    for there in (up, down, right, left):
        pl.semaphore_signal(barrier, inc=1, device_id=there, device_id_type=MESH)
    pl.semaphore_wait(barrier, 4)
    load_own.wait()

    sent = []

    def send(source, target, sems, kind, n, there):
        copy = pltpu.make_async_remote_copy(
            src_ref=source,
            dst_ref=target,
            send_sem=sems.at[0, kind, n],
            recv_sem=sems.at[1, kind, n],
            device_id=there,
            device_id_type=MESH,
        )
        copy.start()
        sent.append(copy)
        return copy

    slab_in = []
    for n, chunk in enumerate(IN_CHUNKS):
        lo, hi = comps_of(chunk)
        slab_in.append(
            (
                send(own.at[2:4, lo:hi], slab.at[0:2, lo:hi], in_sem, 0, n, up),
                send(own.at[0:2, lo:hi], slab.at[2:4, lo:hi], in_sem, 1, n, down),
            )
        )
    for copy in weights:
        copy.start()
    expand_rotations(table_ref, turn_ref, padded, grid_map, into, outof)
    cells = cell_numbers((160, EDGES), 0)
    to_target = jnp.where(cells == target_ref[...], 1.0, 0.0)
    both = to_target + jnp.where(cells == source_ref[...], 1.0, 0.0)
    gather_map[...] = both.T.astype(BF)

    def send_rim(n):
        for copy in slab_in[n]:
            copy.wait_recv()
        take = rim_map((32, 128), 1)
        for step in steps_of(IN_CHUNKS[n]):
            tall = [
                jnp.concatenate([own[:, c].reshape(64, 128), slab[:, c].reshape(64, 128)], 0)
                for c in step
            ]
            got = dot(take, jnp.concatenate(tall, 1)).astype(BF)
            for k, c in enumerate(step):
                rim[0, c] = got[:16, 128 * k : 128 * k + 128]
                rim[1, c] = got[16:, 128 * k : 128 * k + 128]
        lo, hi = comps_of(IN_CHUNKS[n])
        return (
            send(rim.at[0, lo:hi], side.at[0, lo:hi], in_sem, 2, n, right),
            send(rim.at[1, lo:hi], side.at[1, lo:hi], in_sem, 3, n, left),
        )

    def gather(chunk):
        for step in steps_of(chunk):
            pieces = [
                jnp.concatenate(
                    [
                        own[:, c].reshape(64, 128),
                        slab[:, c].reshape(64, 128),
                        side[0, c],
                        side[1, c],
                    ],
                    0,
                )
                for c in step
            ]
            total = dot(gather_map[...], jnp.concatenate(pieces, 1)).astype(BF)
            for k, c in enumerate(step):
                edges[c] = total[:, 128 * k : 128 * k + 128]

    def turn_in(chunk):
        def group_pair(pair, carry):
            for group in (2 * pair, 2 * pair + 1):
                at = pl.ds(pl.multiple_of(group * GROUP, GROUP), GROUP)
                low = pl.ds(pl.multiple_of(EDGES + group * GROUP, GROUP), GROUP)
                for degree in range(chunk[0], chunk[1] + 1):
                    width = 2 * degree + 1
                    n = kept(degree)
                    values = edges[degree * degree : degree * degree + width, at, :]
                    result = dot(
                        into[degree][:, at, :].reshape(n * GROUP, -1)[:, : width * GROUP],
                        values.reshape(width * GROUP, 128),
                    )
                    result = result * (1.0 / math.sqrt(width))
                    piece = [result[GROUP * k : GROUP * k + GROUP] for k in range(n)]
                    mid = n // 2
                    zero_in[at, 128 * degree : 128 * degree + 128] = piece[mid].astype(BF)
                    for m, ref, half in ((1, one_in, 768), (2, two_in, 640)):
                        if degree < m:
                            continue
                        c = 128 * (degree - m)
                        plus, minus = piece[mid + m].astype(BF), piece[mid - m]
                        ref[at, c : c + 128] = plus
                        ref[at, half + c : half + c + 128] = (-minus).astype(BF)
                        ref[low, c : c + 128] = minus.astype(BF)
                        ref[low, half + c : half + c + 128] = plus
            return carry

        lax.fori_loop(0, GROUPS // 2, group_pair, 0)

    side_in = [send_rim(0)]
    for n, chunk in enumerate(IN_CHUNKS):
        if n + 1 < len(IN_CHUNKS):
            side_in.append(send_rim(n + 1))
        for copy in side_in[n]:
            copy.wait_recv()
        gather(chunk)
        turn_in(chunk)

    for copy in weights[:3]:
        copy.wait()
    y0 = dot(zero_in[...], w0[...])
    scalar = y0[:, :128]
    gate = jax.nn.sigmoid(scalar)
    y1 = dot(one_in[...], w1[...])
    zero_in[:, :128] = (scalar * gate).astype(BF)
    for degree in range(1, DEGREE + 1):
        c = 128 * degree
        zero_in[:, c : c + 128] = (y0[:, c : c + 128] * gate).astype(BF)
    y2 = dot(two_in[...], w2[...])
    for y, ref, half in ((y1, one_in, 768), (y2, two_in, 640)):
        for c in range(0, half, 128):
            plus = y[:EDGES, c : c + 128] * gate
            minus = y[EDGES:, c : c + 128] * gate
            ref[:EDGES, c : c + 128] = plus.astype(BF)
            ref[:EDGES, half + c : half + c + 128] = (-minus).astype(BF)
            ref[EDGES:, c : c + 128] = minus.astype(BF)
            ref[EDGES:, half + c : half + c + 128] = plus.astype(BF)
    for copy in weights[3:]:
        copy.wait()

    def second(chunk):
        for m, ref, w in ((0, zero_in, w3), (1, one_in, w4), (2, two_in, w5)):
            first = max(chunk[0], m)
            u = dot(ref[...], w[:, 128 * (first - m) : 128 * (chunk[1] + 1 - m)])
            for degree in range(first, chunk[1] + 1):
                scale = 1.0 / math.sqrt(2 * degree + 1)
                at = FIRST_KEPT[degree] + spread_of(degree)
                c = 128 * (degree - first)
                turned[at + m] = (u[:EDGES, c : c + 128] * scale).astype(BF)
                if m:
                    turned[at - m] = (u[EDGES:, c : c + 128] * scale).astype(BF)

    def turn_out(chunk):
        def group_pair(pair, carry):
            for group in (2 * pair, 2 * pair + 1):
                at = pl.ds(pl.multiple_of(group * GROUP, GROUP), GROUP)
                for degree in range(chunk[0], chunk[1] + 1):
                    first, width, n = FIRST_KEPT[degree], 2 * degree + 1, kept(degree)
                    result = dot(
                        outof[degree * degree : degree * degree + width, at, :]
                        .reshape(width * GROUP, 128)[:, : n * GROUP],
                        turned[first : first + n, at, :].reshape(n * GROUP, 128),
                    )
                    edges[degree * degree : degree * degree + width, at, :] = result.astype(
                        BF
                    ).reshape(width, GROUP, 128)
            return carry

        lax.fori_loop(0, GROUPS // 2, group_pair, 0)

    lane = lax.broadcasted_iota(jnp.int32, (160, EDGES), 1)
    cells = cell_numbers((160, EDGES), 0)
    scatter = jnp.where(
        (cells == target_ref[...]) & (lane < count_ref[0, 0]), 1.0, 0.0
    ).astype(BF)

    def deposit(n):
        for step in steps_of(OUT_CHUNKS[n]):
            total = dot(scatter, jnp.concatenate([edges[c] for c in step], 1))
            for k, c in enumerate(step):
                part = total[:, 128 * k : 128 * k + 128]
                summed[c] = part[:128]
                side_out[0, c] = part[128:144].astype(BF)
                side_out[1, c] = part[144:160].astype(BF)
        lo, hi = comps_of(OUT_CHUNKS[n])
        return (
            send(side_out.at[0, lo:hi], side_back.at[0, lo:hi], out_sem, 0, n, left),
            send(side_out.at[1, lo:hi], side_back.at[1, lo:hi], out_sem, 1, n, right),
        )

    def add_side(n):
        for copy in side_ret[n]:
            copy.wait_recv()
        spread = rim_map((128, 32), 0)
        for step in steps_of(OUT_CHUNKS[n]):
            got = jnp.concatenate(
                [jnp.concatenate([side_back[0, c], side_back[1, c]], 0) for c in step], 1
            )
            extra = dot(spread, got)
            for k, c in enumerate(step):
                total = summed[c] + extra[:, 128 * k : 128 * k + 128]
                summed[c, :64] = total[:64]
                slab_out[:, c] = total[64:].astype(BF).reshape(4, 16, 128)
        lo, hi = comps_of(OUT_CHUNKS[n])
        return (
            send(slab_out.at[0:2, lo:hi], slab_back.at[2:4, lo:hi], out_sem, 2, n, down),
            send(slab_out.at[2:4, lo:hi], slab_back.at[0:2, lo:hi], out_sem, 3, n, up),
        )

    side_ret, slab_ret = [], []
    for n, chunk in enumerate(OUT_CHUNKS):
        second(chunk)
        turn_out(chunk)
        side_ret.append(deposit(n))
        if n:
            slab_ret.append(add_side(n - 1))
    slab_ret.append(add_side(len(OUT_CHUNKS) - 1))
    for n, chunk in enumerate(OUT_CHUNKS):
        for copy in slab_ret[n]:
            copy.wait_recv()
        for c in range(*comps_of(chunk)):
            total = summed[c, :64] + slab_back[:, c].reshape(64, 128).astype(F32)
            out[:, c] = total.astype(BF).reshape(4, 16, 128)
    for copy in sent:
        copy.wait_send()


def fused(own, source, target, turn, count, table, weights):
    vmem = pl.BlockSpec(memory_space=pltpu.VMEM)
    smem = pl.BlockSpec(memory_space=pltpu.SMEM)
    anywhere = pl.BlockSpec(memory_space=pl.ANY)
    into = [
        pltpu.VMEM((kept(d), EDGES, 128 if d <= 3 else 256), BF) for d in range(DEGREE + 1)
    ]
    return pl.pallas_call(
        fused_kernel,
        out_shape=jax.ShapeDtypeStruct((4, COMPS, 16, 128), BF),
        in_specs=[anywhere] + [vmem] * 3 + [smem, vmem] + [anywhere] * 6,
        out_specs=vmem,
        scratch_shapes=[
            pltpu.VMEM((4, COMPS, 16, 128), BF),
            pltpu.VMEM((4, COMPS, 16, 128), BF),
            pltpu.VMEM((2, COMPS, 16, 128), BF),
            pltpu.VMEM((2, COMPS, 16, 128), BF),
        ]
        + [pltpu.VMEM(w.shape, BF) for w in weights]
        + [pltpu.VMEM((EDGES, 1024), BF), pltpu.VMEM((128, 2048), BF)]
        + into
        + [
            pltpu.VMEM((COMPS, EDGES, 128), BF),
            pltpu.VMEM((EDGES, 160), BF),
            pltpu.VMEM((COMPS, EDGES, 128), BF),
            pltpu.VMEM((EDGES, 896), BF),
            pltpu.VMEM((2 * EDGES, 1536), BF),
            pltpu.VMEM((2 * EDGES, 1280), BF),
            pltpu.VMEM((FIRST_KEPT[-1], EDGES, 128), BF),
            pltpu.VMEM((COMPS, 128, 128), F32),
            pltpu.VMEM((2, COMPS, 16, 128), BF),
            pltpu.VMEM((2, COMPS, 16, 128), BF),
            pltpu.VMEM((4, COMPS, 16, 128), BF),
            pltpu.VMEM((4, COMPS, 16, 128), BF),
            pltpu.SemaphoreType.DMA((7,)),
            pltpu.SemaphoreType.DMA((2, 4, len(IN_CHUNKS))),
            pltpu.SemaphoreType.DMA((2, 4, len(OUT_CHUNKS))),
        ],
        compiler_params=pltpu.CompilerParams(
            vmem_limit_bytes=52 * 1024 * 1024, collective_id=0, has_side_effects=True
        ),
        cost_estimate=pl.CostEstimate(
            flops=12_000_000_000, bytes_accessed=20_000_000, transcendentals=40_000
        ),
        name="edge_messages",
    )(own, source, target, turn, count, table, *weights)


def shards(features, source_cell, target_cell, rotation, edge_count, *weights):
    own = jnp.transpose(features, (0, 2, 1, 3))
    turn = jnp.transpose(rotation[0, 0], (2, 0, 1)).reshape(WIGNER, EDGES)
    weights = [w.reshape(-1, w.shape[-1]) for w in weights]
    result = fused(
        own,
        source_cell.reshape(1, EDGES),
        target_cell.reshape(1, EDGES),
        turn,
        edge_count,
        jnp.asarray(entry_tables()),
        weights,
    )
    return jnp.transpose(result, (0, 2, 1, 3))


def solution(mesh):
    return jax.shard_map(
        shards,
        mesh=mesh,
        in_specs=(
            P("slab", "sub", None, None),
            P("slab", "sub", None, None),
            P("slab", "sub", None, None),
            P("slab", "sub", None, None, None),
            P("slab", "sub"),
            P(),
            P(),
            P(),
            P(),
            P(),
            P(),
        ),
        out_specs=P("slab", "sub", None, None),
        check_vma=False,
    )
```
